256 devices in a mesh: gx: 8 (over x_hi, y), gy: 4 (over x_lo, core), gz: 8 (over z).
Axes of the slice: x: 4 (x_hi: 2, x_lo: 2; x = x_hi * 2 + x_lo), y: 4, z: 8, core: 2. Of those that a mesh axis runs over, the one named last changes fastest.
Arguments:
- node_latents: bfloat16 [262144, 128], P(('gx', 'gy', 'gz')), may hold values from -300 to 300
- cluster_latents: bfloat16 [65536, 128], P(('gx', 'gy', 'gz')), may hold values from -6 to 6
- senders: int32 [8192, 128], P(('gx', 'gy', 'gz')), may hold values from 0 to 4095
- membership: int32 [262144], P(('gx', 'gy', 'gz')), may hold values from 0 to 255
- w_key: bfloat16 [128, 128], replicated, may hold values from -1 to 1
- w_value: bfloat16 [128, 128], replicated, may hold values from -0.5 to 0.5
- w_edge_in: bfloat16 [256, 128], replicated, may hold values from -0.375 to 0.375
- w_edge_out: bfloat16 [128, 128], replicated, may hold values from -0.5 to 0.5
- w_node_in: bfloat16 [512, 128], replicated, may hold values from -0.25 to 0.25
- w_node_out: bfloat16 [128, 128], replicated, may hold values from -0.5 to 0.5
- out_gain: float32 [128], replicated, may hold values from 0.5 to 1.5
Outputs:
- new_latents: bfloat16 [262144, 128], P(('gx', 'gy', 'gz'))
The draws below stay inside these ranges and needn't reach their ends.
All inputs are finite; a program needn't handle non-finite values.
Results may differ from the reference program's by a relative error of at most 0.005.
Values may be sent and summed in bfloat16 or wider, within the bound.
No kernel may reach another device: no remote copies, remote signals or barrier semaphores. Data moves between devices by JAX's collectives and lax.ppermute only.
A program may use at most 64 MiB of HBM per device.

```python
import jax
import jax.numpy as jnp
from jax import lax

H = 128
NODES_DEV = 1024
CL_DEV = 256
BND = 512
DEG = 4
EDGE_ROWS = 32
NODES = 262144
CLUSTERS = 65536
N_GX = 8
N_GY = 4
N_GZ = 8
DEVICES = 256


def shared_parts(key):
    cluster_key, weight_key = jax.random.split(jax.random.fold_in(key, 7))
    clusters = jnp.clip(jax.random.normal(cluster_key, (CLUSTERS, H), jnp.float32), -6.0, 6.0)
    weights = jnp.clip(jax.random.normal(weight_key, (H, H), jnp.float32), -6.0, 6.0) / jnp.sqrt(jnp.float32(H))
    return (clusters, weights)


def draw_cluster_latents(key, part):
    return shared_parts(key)[0].astype(jnp.bfloat16)


def draw_w_key(key, part):
    return shared_parts(key)[1].astype(jnp.bfloat16)


def draw_node_latents(key, part):
    base_key = jax.random.fold_in(key, 11)
    latents = jnp.clip(jax.random.normal(base_key, (NODES, H), jnp.float32), -6.0, 6.0)
    return latents.astype(jnp.bfloat16)


def plant(drawn, own_key, least, top_value):
    longest = drawn.shape.index(max(drawn.shape))
    spots = []
    for shift in (0, 1):
        where = [jax.random.randint(jax.random.fold_in(own_key, axis), (), 0, length) for axis, length in enumerate(drawn.shape)]
        where[longest] = (where[longest] + shift) % drawn.shape[longest]
        spots.append(tuple(where))
    return drawn.at[spots[0]].set(least).at[spots[1]].set(top_value)


def normal_values(rng, shape, scale, bound, kind=jnp.bfloat16):
    return jnp.clip(scale * jax.random.normal(rng, shape, jnp.float32), -bound, bound).astype(kind)


def setup_inputs(seed: int = 0) -> dict:
    splits = jax.random.split(jax.random.key(seed), 12)
    node_latents = draw_node_latents(jax.random.fold_in(splits[11], 71), 0)
    cluster_latents = draw_cluster_latents(jax.random.fold_in(splits[11], 71), 0)
    senders = plant(jax.random.randint(splits[2], (DEVICES * EDGE_ROWS, 128), 0, NODES_DEV + 6 * BND), jax.random.fold_in(splits[2], 1), 0, (NODES_DEV + 6 * BND) - 1).astype(jnp.int32)
    membership = plant(jax.random.randint(splits[3], (NODES,), 0, CL_DEV), jax.random.fold_in(splits[3], 1), 0, CL_DEV - 1).astype(jnp.int32)
    w_key = draw_w_key(jax.random.fold_in(splits[11], 71), 0)
    w_value = normal_values(splits[5], (H, H), H ** -0.5, 0.5)
    w_edge_in = normal_values(splits[6], (2 * H, H), (2 * H) ** -0.5, 0.375)
    w_edge_out = normal_values(splits[7], (H, H), H ** -0.5, 0.5)
    w_node_in = normal_values(splits[8], (4 * H, H), (4 * H) ** -0.5, 0.25)
    w_node_out = normal_values(splits[9], (H, H), H ** -0.5, 0.5)
    out_gain = jnp.clip(1.0 + 0.1 * jax.random.normal(splits[10], (H,), jnp.float32), 0.5, 1.5)
    return dict(node_latents=node_latents, cluster_latents=cluster_latents, senders=senders, membership=membership, w_key=w_key, w_value=w_value, w_edge_in=w_edge_in, w_edge_out=w_edge_out, w_node_in=w_node_in, w_node_out=w_node_out, out_gain=out_gain)


def project(latent_rows, weight):
    return jnp.dot(latent_rows, weight, preferred_element_type=jnp.float32).astype(jnp.bfloat16)

def attend(queries, key_rows, value_rows):
    scores = jnp.dot(queries, key_rows.T, preferred_element_type=jnp.float32) / jnp.sqrt(jnp.float32(queries.shape[1]))
    highest = lax.optimization_barrier(jnp.max(scores, axis=1, keepdims=True))
    exponent = jnp.exp(scores - highest)
    numer = jnp.dot(exponent.astype(jnp.bfloat16), value_rows, preferred_element_type=jnp.float32)
    return numer / lax.optimization_barrier(jnp.sum(exponent, axis=1, keepdims=True))

def reference(node_latents, cluster_latents, senders, membership, w_key, w_value, w_edge_in, w_edge_out, w_node_in, w_node_out, out_gain):
    width = node_latents.shape[1]
    key_grid = project(cluster_latents, w_key).reshape(N_GX, N_GY, N_GZ, CL_DEV, width)
    value_grid = project(cluster_latents, w_value).reshape(N_GX, N_GY, N_GZ, CL_DEV, width)
    cluster_grid = cluster_latents.reshape(N_GX, N_GY, N_GZ, CL_DEV, width)
    node_grid = node_latents.reshape(N_GX, N_GY, N_GZ, NODES_DEV, width)
    border = node_grid[:, :, :, :BND]
    faces = jnp.stack([jnp.roll(border, 1, axis=0), jnp.roll(border, -1, axis=0), jnp.roll(border, 1, axis=1), jnp.roll(border, -1, axis=1), jnp.roll(border, 1, axis=2), jnp.roll(border, -1, axis=2)], axis=3)
    faces = faces.reshape(N_GX, N_GY, N_GZ, 6 * BND, width)
    edge_grid = senders.reshape(N_GX, N_GY, N_GZ, NODES_DEV * DEG)
    member_grid = membership.reshape(N_GX, N_GY, N_GZ, NODES_DEV)

    def one_block(device_flat):
        index_x = device_flat // (N_GY * N_GZ)
        index_y = device_flat // N_GZ % N_GY
        index_z = device_flat % N_GZ
        own = node_grid[index_x, index_y, index_z]
        pooled = attend(own, key_grid[:, index_y, index_z].reshape(-1, width), value_grid[:, index_y, index_z].reshape(-1, width))
        pooled = pooled + attend(own, key_grid[index_x, :, index_z].reshape(-1, width), value_grid[index_x, :, index_z].reshape(-1, width))
        pooled = pooled + attend(own, key_grid[index_x, index_y].reshape(-1, width), value_grid[index_x, index_y].reshape(-1, width))
        attended = (pooled * lax.rsqrt(lax.optimization_barrier(jnp.mean(pooled * pooled, axis=1, keepdims=True)) + 1e-06)).astype(jnp.bfloat16)
        extended = jnp.concatenate([own, faces[index_x, index_y, index_z]], axis=0)
        sender_rows = jnp.take(extended, edge_grid[index_x, index_y, index_z], axis=0)
        receiver_part = jnp.dot(own, w_edge_in[:width], preferred_element_type=jnp.float32)
        sender_part = jnp.dot(sender_rows, w_edge_in[width:], preferred_element_type=jnp.float32)
        edge_hidden = jax.nn.silu(sender_part.reshape(NODES_DEV, DEG, width) + receiver_part[:, None, :]).astype(jnp.bfloat16)
        messages = jnp.dot(edge_hidden.reshape(NODES_DEV * DEG, width), w_edge_out, preferred_element_type=jnp.float32)
        aggregated = lax.optimization_barrier(jnp.sum(messages.reshape(NODES_DEV, DEG, width), axis=1)).astype(jnp.bfloat16)
        own_cluster = jnp.take(cluster_grid[index_x, index_y, index_z], member_grid[index_x, index_y, index_z], axis=0)
        preact = jnp.dot(own, w_node_in[:width], preferred_element_type=jnp.float32)
        preact = preact + jnp.dot(aggregated, w_node_in[width:2 * width], preferred_element_type=jnp.float32)
        preact = preact + jnp.dot(attended, w_node_in[2 * width:3 * width], preferred_element_type=jnp.float32)
        preact = preact + jnp.dot(own_cluster, w_node_in[3 * width:], preferred_element_type=jnp.float32)
        node_hidden = jax.nn.silu(preact).astype(jnp.bfloat16)
        update = jnp.dot(node_hidden, w_node_out, preferred_element_type=jnp.float32)
        centred = update - lax.optimization_barrier(jnp.mean(update, axis=1, keepdims=True))
        variance = lax.optimization_barrier(jnp.mean(centred * centred, axis=1, keepdims=True))
        normed = centred * lax.rsqrt(variance + 1e-05)
        return (own.astype(jnp.float32) + normed * out_gain).astype(jnp.bfloat16)
    blocks = lax.map(one_block, jnp.arange(N_GX * N_GY * N_GZ, dtype=jnp.int32))
    return blocks.reshape(-1, width)
```

```python
import math

import jax
import jax.numpy as jnp
from jax import lax
from jax.experimental import pallas as pl
from jax.experimental.pallas import tpu as pltpu
from jax.sharding import PartitionSpec as P

BND = 512
F32 = jnp.float32
BF16 = jnp.bfloat16
TILE = 128
ROWS = 256
CHUNK = 512

VMEM = pl.BlockSpec(memory_space=pltpu.VMEM)
SMEM = pl.BlockSpec(memory_space=pltpu.SMEM)


def dot(a, b):
    return jnp.dot(a, b, preferred_element_type=F32)


def silu(x):
    return x * 0.5 * (1.0 + jnp.tanh(x * 0.5))


def edge_kernel(
    senders, own, xa, xb, ya, yb, za, zb, member, clusters, w_in, w_out, w_node, base, table, recv, rows
):
    count, width = own.shape
    w_send = w_in[width:, :]
    table[0:count, :] = dot(own[...], w_send)
    at = count
    for face in (xa, xb, ya, yb, za, zb):
        table[at : at + BND, :] = dot(face[...], w_send)
        at += BND
    recv[...] = dot(own[...], w_in[:width, :])
    w_sum = jnp.concatenate([w_out[...]] * 4, axis=0)
    lanes = lax.broadcasted_iota(jnp.int32, (TILE, clusters.shape[0]), 1)
    columns = member[...].T

    for t in range(count // TILE):

        def gather(g, _, t=t):
            for j in range(16):
                for d in range(4):
                    index = senders[t * TILE * 4 + g * 64 + j * 4 + d]
                    rows[d, pl.ds(pl.multiple_of(g * 16, 16) + j, 1), :] = table[pl.ds(index, 1), :]
            return 0

        lax.fori_loop(0, TILE // 16, gather, 0)
        here = pl.ds(t * TILE, TILE)
        r = recv[here, :]
        hidden = jnp.concatenate([silu(rows[d] + r).astype(BF16) for d in range(4)], axis=1)
        agg = dot(hidden, w_sum).astype(BF16)
        one_hot = (columns[:, t : t + 1] == lanes).astype(BF16)
        own_cluster = dot(one_hot, clusters[...]).astype(BF16)
        base[here, :] = (
            dot(own[here, :], w_node[:width, :])
            + dot(agg, w_node[width : 2 * width, :])
            + dot(own_cluster, w_node[3 * width :, :])
        )


def project_pieces(pieces, w_key, w_value, keys, values):
    at = 0
    for piece in pieces:
        n, width = piece.shape
        keys[:, at : at + n] = dot(piece[...], w_key[...]).astype(BF16).T
        values[at : at + n, 0:width] = dot(piece[...], w_value[...]).astype(BF16)
        values[at : at + n, width : 2 * width] = jnp.ones((n, width), BF16)
        at += n


def attend_rows(q, keys, values, scale):
    total = values.shape[0]
    width = q.shape[1]
    top = acc = None
    for at in range(0, total, CHUNK):
        scores = dot(q, keys[:, at : at + CHUNK])
        highest = jnp.max(scores, axis=1, keepdims=True)
        newest = highest if top is None else jnp.maximum(top, highest)
        weights = jnp.exp2((scores - newest) * scale).astype(BF16)
        part = dot(weights, values[at : at + CHUNK, :])
        acc = part if acc is None else acc * jnp.exp2((top - newest) * scale) + part
        top = newest
    return acc[:, :width] / acc[:, width:]


def score_scale(width):
    return math.log2(math.e) / math.sqrt(width)


def line_kernel(queries, *refs):
    *pieces, w_key, w_value, out, keys, values = refs
    project_pieces(pieces, w_key, w_value, keys, values)
    scale = score_scale(queries.shape[1])

    def step(r, _):
        here = pl.ds(pl.multiple_of(r * ROWS, ROWS), ROWS)
        out[here, :] = attend_rows(queries[here, :], keys, values, scale)
        return 0

    lax.fori_loop(0, queries.shape[0] // ROWS, step, 0)


def final_kernel(queries, *refs):
    *pieces, w_key, w_value, line_x, line_y, base, w_node, w_out, gain, out, keys, values = refs
    project_pieces(pieces, w_key, w_value, keys, values)
    width = queries.shape[1]
    scale = score_scale(width)

    def step(r, _):
        here = pl.ds(pl.multiple_of(r * ROWS, ROWS), ROWS)
        pooled = line_x[here, :] + line_y[here, :] + attend_rows(queries[here, :], keys, values, scale)
        attended = (
            pooled * lax.rsqrt(jnp.mean(pooled * pooled, axis=1, keepdims=True) + 1e-06)
        ).astype(BF16)
        preact = base[here, :] + dot(attended, w_node[2 * width : 3 * width, :])
        update = dot(silu(preact).astype(BF16), w_out[...])
        centred = update - jnp.mean(update, axis=1, keepdims=True)
        variance = jnp.mean(centred * centred, axis=1, keepdims=True)
        normed = centred * lax.rsqrt(variance + 1e-05)
        out[here, :] = (queries[here, :].astype(F32) + normed * gain[...]).astype(BF16)
        return 0

    lax.fori_loop(0, queries.shape[0] // ROWS, step, 0)


def exchange(x, axis, distance):
    return lax.ppermute(x, axis, [(i, i ^ distance) for i in range(lax.axis_size(axis))])


def line_pieces(block, axis, distances):
    pieces = [block]
    held = block
    for at, distance in enumerate(distances):
        came = exchange(held, axis, distance)
        pieces.append(came)
        if at + 1 < len(distances):
            held = jnp.concatenate([held, came], axis=0)
    return pieces


def shifted(x, axis, by):
    size = lax.axis_size(axis)
    return lax.ppermute(x, axis, [(i, (i + by) % size) for i in range(size)])


def on_device(
    node_latents,
    cluster_latents,
    senders,
    membership,
    w_key,
    w_value,
    w_edge_in,
    w_edge_out,
    w_node_in,
    w_node_out,
    out_gain,
):
    count, width = node_latents.shape
    border = node_latents[:BND]
    faces = [shifted(border, axis, by) for axis in ("gx", "gy", "gz") for by in (1, -1)]
    along_z = line_pieces(cluster_latents, "gz", (4, 2, 1))
    along_x = line_pieces(cluster_latents, "gx", (2, 4, 1))
    along_y = line_pieces(cluster_latents, "gy", (1, 2))

    base = pl.pallas_call(
        edge_kernel,
        out_shape=jax.ShapeDtypeStruct((count, width), F32),
        in_specs=[SMEM] + [VMEM] * 12,
        out_specs=VMEM,
        scratch_shapes=[
            pltpu.VMEM((count + 6 * BND, width), F32),
            pltpu.VMEM((count, width), F32),
            pltpu.VMEM((4, TILE, width), F32),
        ],
        name="edges",
    )(
        senders.reshape(-1),
        node_latents,
        *faces,
        membership.reshape(count // TILE, TILE),
        cluster_latents,
        w_edge_in,
        w_edge_out,
        w_node_in,
    )

    def keys_and_values(pieces):
        total = sum(p.shape[0] for p in pieces)
        return [pltpu.VMEM((width, total), BF16), pltpu.VMEM((total, 2 * width), BF16)]

    def line(pieces, name):
        return pl.pallas_call(
            line_kernel,
            out_shape=jax.ShapeDtypeStruct((count, width), F32),
            in_specs=[VMEM] * (3 + len(pieces)),
            out_specs=VMEM,
            scratch_shapes=keys_and_values(pieces),
            name=name,
        )(node_latents, *pieces, w_key, w_value)

    line_y = line(along_y, "line_y")
    line_x = line(along_x, "line_x")
    return pl.pallas_call(
        final_kernel,
        out_shape=jax.ShapeDtypeStruct((count, width), BF16),
        in_specs=[VMEM] * (9 + len(along_z)),
        out_specs=VMEM,
        scratch_shapes=keys_and_values(along_z),
        name="final",
    )(
        node_latents,
        *along_z,
        w_key,
        w_value,
        line_x,
        line_y,
        base,
        w_node_in,
        w_node_out,
        out_gain.reshape(1, width),
    )


def solution(mesh):
    split = P(("gx", "gy", "gz"), None)
    in_specs = (split, split, split, P(("gx", "gy", "gz"))) + (P(),) * 7
    return jax.shard_map(
        on_device, mesh=mesh, in_specs=in_specs, out_specs=split, check_vma=False
    )
```

```python
import math

import jax
import jax.numpy as jnp
from jax import lax
from jax.experimental import pallas as pl
from jax.experimental.pallas import tpu as pltpu
from jax.sharding import PartitionSpec as P


BND = 512
F32 = jnp.float32
BF16 = jnp.bfloat16
TILE = 128
ROWS = 256
VMEM_BYTES = 20 * 2**20

VMEM = pl.BlockSpec(memory_space=pltpu.VMEM)
SMEM = pl.BlockSpec(memory_space=pltpu.SMEM)

W_KEY, W_VALUE, _, W_SEND, W_MSG, _, W_AGG, W_ATT, _, W_OUT = range(10)


def near(x):
    return pltpu.with_memory_space_constraint(x, pltpu.VMEM)


def dot(a, b):
    return jnp.dot(a, b, preferred_element_type=F32)


def silu(x):
    return x * 0.5 * (1.0 + jnp.tanh(x * 0.5))


def weight(stacked, which):
    width = stacked.shape[1]
    return stacked[which * width : (which + 1) * width, :]


def scale_of(width):
    return math.log2(math.e) / math.sqrt(width)


def row_loop(count, body):
    def step(r, _):
        body(pl.ds(pl.multiple_of(r * ROWS, ROWS), ROWS))
        return 0

    lax.fori_loop(0, count // ROWS, step, 0)


def project(pieces, weights, keys, values):
    width = weights.shape[1]
    at = 0
    for piece in pieces:
        n = piece.shape[0]
        keys[:, at : at + n] = dot(piece[...], weight(weights, W_KEY)).astype(BF16).T
        values[at : at + n, 0:width] = dot(piece[...], weight(weights, W_VALUE)).astype(BF16)
        values[at : at + n, width : 2 * width] = jnp.ones((n, width), BF16)
        at += n


def wide(x, copies):
    return jnp.concatenate([x] * copies, axis=1)


def absorb(q, keys, values, top, acc):
    width = q.shape[1]
    scale = scale_of(width)
    scores = dot(q, keys)
    highest = jnp.broadcast_to(jnp.max(scores, axis=1, keepdims=True), (q.shape[0], width))
    newest = highest if top is None else jnp.maximum(top, highest)
    weights = jnp.exp2((scores - wide(newest, scores.shape[1] // width)) * scale).astype(BF16)
    part = dot(weights, values)
    if top is not None:
        part = acc * wide(jnp.exp2((top - newest) * scale), 2) + part
    return newest, part


def load_kernel(
    own_far, clusters_far, member_far, gain_far, own, clusters, border, both, member, gain, done
):
    head = own_far.at[:BND, :]
    copies = [
        pltpu.make_async_copy(source, target, done.at[at])
        for at, (source, target) in enumerate(
            (
                (head, both.at[:BND, :]),
                (clusters_far, both.at[BND:, :]),
                (head, border),
                (clusters_far, clusters),
                (member_far, member),
                (gain_far, gain),
                (own_far, own),
            )
        )
    ]
    for copy in copies:
        copy.start()
    for copy in copies:
        copy.wait()


def stack_kernel(*refs):
    *pieces, out = refs
    at = 0
    for piece in pieces:
        out[at : at + piece.shape[0], :] = piece[...]
        at += piece.shape[0]


def stack_after_border_kernel(border, clusters, came, out):
    n = clusters.shape[0]
    out[:BND, :] = border[...]
    out[BND : BND + n, :] = clusters[...]
    out[BND + n :, :] = came[BND:, :]


def prep_kernel(
    own, clusters, member, w_key, w_value, w_in, w_msg, w_node, w_out,
    weights, recv, base, top, acc, keys, values,
):
    count, width = own.shape
    at = 0
    for w in (w_key, w_value, w_in, w_msg, w_node, w_out):
        weights[at : at + w.shape[0], :] = w[...]
        at += w.shape[0]
    project((clusters,), weights, keys, values)
    columns = member[...].T
    lanes = lax.broadcasted_iota(jnp.int32, (TILE, clusters.shape[0]), 1)
    for t in range(count // TILE):
        here = pl.ds(t * TILE, TILE)
        q = own[here, :]
        one_hot = (columns[:, t : t + 1] == lanes).astype(BF16)
        own_cluster = dot(one_hot, clusters[...]).astype(BF16)
        base[here, :] = dot(q, weight(w_node, 0)) + dot(own_cluster, weight(w_node, 3))
        recv[here, :] = dot(q, w_in[:width, :])
        top[here, :], acc[here, :] = absorb(q, keys[...], values[...], None, None)


def edge_kernel(senders, own, xa, xb, ya, yb, za, zb, weights, recv, base, out, table, rows):
    count, _ = own.shape
    w_send = weight(weights, W_SEND)
    table[0:count, :] = dot(own[...], w_send)
    for at, axis, pair in ((0, "gx", (xa, xb)), (2, "gy", (ya, yb)), (4, "gz", (za, zb))):
        odd = lax.axis_index(axis) % 2
        low = pl.multiple_of(count + BND * (at + 1 - odd), BND)
        high = pl.multiple_of(count + BND * (at + odd), BND)
        table[pl.ds(low, BND), :] = dot(pair[0][:BND, :], w_send)
        table[pl.ds(high, BND), :] = dot(pair[1][:BND, :], w_send)
    w_sum = jnp.concatenate([weight(weights, W_MSG)] * 4, axis=0)

    def tile(t, _):
        def gather(g, _):
            for j in range(16):
                for d in range(4):
                    index = senders[t * TILE * 4 + g * 64 + j * 4 + d]
                    rows[d, pl.ds(pl.multiple_of(g * 16, 16) + j, 1), :] = table[pl.ds(index, 1), :]
            return 0

        lax.fori_loop(0, TILE // 16, gather, 0)
        here = pl.ds(pl.multiple_of(t * TILE, TILE), TILE)
        r = recv[here, :]
        hidden = jnp.concatenate([silu(rows[d] + r).astype(BF16) for d in range(4)], axis=1)
        agg = dot(hidden, w_sum).astype(BF16)
        out[here, :] = base[here, :] + dot(agg, weight(weights, W_AGG))
        return 0

    lax.fori_loop(0, count // TILE, tile, 0)


def middle_kernel(own, weights, top0, acc0, y0, y1, x0, x1, z0, z1, line_y, top_x, acc_x, top_z, acc_z, keys, values):
    count, width = own.shape
    n = x0.shape[0]
    project((y0.at[BND:, :], y1.at[BND:, :], x0, x1, z0, z1), weights, keys, values)

    def rows(here):
        q = own[here, :]
        t0, a0 = top0[here, :], acc0[here, :]
        _, a = absorb(q, keys[:, 0 : 3 * n], values[0 : 3 * n, :], t0, a0)
        line_y[here, :] = a[:, :width] / a[:, width:]
        top_x[here, :], acc_x[here, :] = absorb(q, keys[:, 3 * n : 6 * n], values[3 * n : 6 * n, :], t0, a0)
        top_z[here, :], acc_z[here, :] = absorb(q, keys[:, 6 * n : 9 * n], values[6 * n : 9 * n, :], t0, a0)

    row_loop(count, rows)


def final_kernel(own, weights, gain, base, line_y, top_x, acc_x, top_z, acc_z, x2, z2, out, keys, values):
    count, width = own.shape
    n = x2.shape[0]
    project((x2, z2), weights, keys, values)

    def rows(here):
        q = own[here, :]
        _, ax = absorb(q, keys[:, 0:n], values[0:n, :], top_x[here, :], acc_x[here, :])
        _, az = absorb(q, keys[:, n : 2 * n], values[n : 2 * n, :], top_z[here, :], acc_z[here, :])
        pooled = line_y[here, :] + ax[:, :width] / ax[:, width:] + az[:, :width] / az[:, width:]
        attended = (
            pooled * lax.rsqrt(jnp.mean(pooled * pooled, axis=1, keepdims=True) + 1e-06)
        ).astype(BF16)
        preact = base[here, :] + dot(attended, weight(weights, W_ATT))
        update = dot(silu(preact).astype(BF16), weight(weights, W_OUT))
        centred = update - jnp.mean(update, axis=1, keepdims=True)
        variance = jnp.mean(centred * centred, axis=1, keepdims=True)
        normed = centred * lax.rsqrt(variance + 1e-05)
        out[here, :] = (q.astype(F32) + normed * gain[...]).astype(BF16)

    row_loop(count, rows)


def call(kernel, args, outs, scratch=(), scalars=(), local=True):
    space = pltpu.VMEM if local else jax.ShapeDtypeStruct
    many = isinstance(outs, list)
    return pl.pallas_call(
        kernel,
        out_shape=[space(*o) for o in outs] if many else space(*outs),
        in_specs=[SMEM] * len(scalars) + [VMEM] * len(args),
        out_specs=[VMEM] * len(outs) if many else VMEM,
        scratch_shapes=[pltpu.VMEM(*s) for s in scratch],
        compiler_params=pltpu.CompilerParams(vmem_limit_bytes=VMEM_BYTES),
    )(*scalars, *map(near, args))


def exchange(x, axis, partner):
    size = lax.axis_size(axis)
    return lax.ppermute(x, axis, [(i, partner(i) % size) for i in range(size)])


def other_side(i):
    return i + 1 if i % 2 else i - 1


def on_device(
    node_latents,
    cluster_latents,
    senders,
    membership,
    w_key,
    w_value,
    w_edge_in,
    w_edge_out,
    w_node_in,
    w_node_out,
    out_gain,
):
    count, width = node_latents.shape
    n = cluster_latents.shape[0]

    def stack(pieces):
        return call(stack_kernel, pieces, ((sum(p.shape[0] for p in pieces), width), BF16))

    z0 = exchange(cluster_latents, "gz", lambda i: i ^ 4)
    x0 = exchange(cluster_latents, "gx", lambda i: i ^ 2)
    own, clusters, border, both, member, gain = pl.pallas_call(
        load_kernel,
        out_shape=[
            pltpu.VMEM((count, width), BF16),
            pltpu.VMEM((n, width), BF16),
            pltpu.VMEM((BND, width), BF16),
            pltpu.VMEM((BND + n, width), BF16),
            pltpu.VMEM((count // TILE, TILE), jnp.int32),
            pltpu.VMEM((1, width), F32),
        ],
        in_specs=[pl.BlockSpec(memory_space=pltpu.HBM)] * 4,
        out_specs=[VMEM] * 6,
        scratch_shapes=[pltpu.SemaphoreType.DMA((7,))],
        compiler_params=pltpu.CompilerParams(vmem_limit_bytes=VMEM_BYTES),
        name="load",
    )(
        *(
            pltpu.with_memory_space_constraint(x, pltpu.HBM)
            for x in (
                node_latents,
                cluster_latents,
                membership.reshape(count // TILE, TILE),
                out_gain.reshape(1, width),
            )
        )
    )
    y0 = exchange(both, "gy", lambda i: i ^ 1)
    za = exchange(border, "gz", lambda i: i ^ 1)
    xa = exchange(border, "gx", lambda i: i ^ 1)
    zb = exchange(border, "gz", other_side)
    xb = exchange(border, "gx", other_side)

    weights, recv, base, top, acc = call(
        prep_kernel,
        (
            own,
            clusters,
            member,
            w_key,
            w_value,
            w_edge_in,
            w_edge_out,
            w_node_in,
            w_node_out,
        ),
        [
            ((10 * width, width), BF16),
            ((count, width), F32),
            ((count, width), F32),
            ((count, width), F32),
            ((count, 2 * width), F32),
        ],
        [((width, n), BF16), ((n, 2 * width), BF16)],
    )

    x1 = exchange(stack((clusters, x0)), "gx", lambda i: i ^ 4)
    y1 = exchange(
        call(stack_after_border_kernel, (border, clusters, y0), ((BND + 2 * n, width), BF16)), "gy", lambda i: i ^ 3
    )
    z1 = exchange(stack((clusters, z0)), "gz", lambda i: i ^ 2)
    z2 = exchange(stack((clusters, z0, z1)), "gz", lambda i: i ^ 1)
    x2 = exchange(stack((clusters, x0, x1)), "gx", lambda i: i ^ 1)

    base = call(
        edge_kernel,
        (own, xa, xb, y0, y1, za, zb, weights, recv, base),
        ((count, width), F32),
        [((count + 6 * BND, width), F32), ((4, TILE, width), F32)],
        (senders.reshape(-1),),
    )
    line_y, top_x, acc_x, top_z, acc_z = call(
        middle_kernel,
        (own, weights, top, acc, y0, y1, x0, x1, z0, z1),
        [((count, width), F32)] + [((count, width), F32), ((count, 2 * width), F32)] * 2,
        [((width, 9 * n), BF16), ((9 * n, 2 * width), BF16)],
    )
    return call(
        final_kernel,
        (own, weights, gain, base, line_y, top_x, acc_x, top_z, acc_z, x2, z2),
        ((count, width), BF16),
        [((width, 8 * n), BF16), ((8 * n, 2 * width), BF16)],
        local=False,
    )


def solution(mesh):
    split = P(("gx", "gy", "gz"), None)
    in_specs = (split, split, split, P(("gx", "gy", "gz"))) + (P(),) * 7

    return jax.shard_map(on_device, mesh=mesh, in_specs=in_specs, out_specs=split, check_vma=False)
```

```python
import math

import jax
import jax.numpy as jnp
from jax import lax
from jax.experimental import pallas as pl
from jax.experimental.pallas import tpu as pltpu
from jax.sharding import PartitionSpec as P


BND = 512
F32 = jnp.float32
BF16 = jnp.bfloat16
TILE = 128
ROWS = 256
NODES_STEP = 64
VMEM_BYTES = 20 * 2**20

VMEM = pl.BlockSpec(memory_space=pltpu.VMEM)
SMEM = pl.BlockSpec(memory_space=pltpu.SMEM)

W_KEY, W_VALUE, _, W_SEND, W_MSG, _, W_AGG, W_ATT, _, W_OUT = range(10)


def near(x):
    return pltpu.with_memory_space_constraint(x, pltpu.VMEM)


def dot(a, b):
    return jnp.dot(a, b, preferred_element_type=F32)


def silu(x):
    return x * 0.5 * (1.0 + jnp.tanh(x * 0.5))


def weight(stacked, which):
    width = stacked.shape[1]
    return stacked[which * width : (which + 1) * width, :]


def scale_of(width):
    return math.log2(math.e) / math.sqrt(width)


def row_tiles(count, rows):
    return [pl.ds(at, rows) for at in range(0, count, rows)]


def project(pieces, weights, keys, values):
    width = weights.shape[1]
    at = 0
    for piece in pieces:
        n = piece.shape[0]
        keys[:, at : at + n] = dot(piece[...], weight(weights, W_KEY)).astype(BF16).T
        values[at : at + n, 0:width] = dot(piece[...], weight(weights, W_VALUE)).astype(BF16)
        values[at : at + n, width : 2 * width] = jnp.ones((n, width), BF16)
        at += n


def wide(x, copies):
    return jnp.concatenate([x] * copies, axis=1)


def absorb(q, keys, values, top, acc):
    width = q.shape[1]
    scale = scale_of(width)
    scores = dot(q, keys)
    highest = jnp.broadcast_to(jnp.max(scores, axis=1, keepdims=True), (q.shape[0], width))
    newest = highest if top is None else jnp.maximum(top, highest)
    weights = jnp.exp2((scores - wide(newest, scores.shape[1] // width)) * scale).astype(BF16)
    part = dot(weights, values)
    if top is not None:
        part = acc * wide(jnp.exp2((top - newest) * scale), 2) + part
    return newest, part


def load_kernel(
    own_far, clusters_far, member_far, gain_far, own, clusters, border, both, member, gain, done
):
    head = own_far.at[:BND, :]
    copies = [
        pltpu.make_async_copy(source, target, done.at[at])
        for at, (source, target) in enumerate(
            (
                (head, both.at[:BND, :]),
                (clusters_far, both.at[BND:, :]),
                (head, border),
                (clusters_far, clusters),
                (member_far, member),
                (gain_far, gain),
                (own_far, own),
            )
        )
    ]
    for copy in copies:
        copy.start()
    for copy in copies:
        copy.wait()


def stack_kernel(*refs):
    *pieces, out = refs
    at = 0
    for piece in pieces:
        out[at : at + piece.shape[0], :] = piece[...]
        at += piece.shape[0]


def stack_after_border_kernel(border, clusters, came, out):
    n = clusters.shape[0]
    out[:BND, :] = border[...]
    out[BND : BND + n, :] = clusters[...]
    out[BND + n :, :] = came[BND:, :]


def prep_kernel(
    own, clusters, member, w_key, w_value, w_in, w_msg, w_node, w_out,
    weights, recv, base, top, acc, keys, values,
):
    count, width = own.shape
    at = 0
    for w in (w_key, w_value, w_in, w_msg, w_node, w_out):
        weights[at : at + w.shape[0], :] = w[...]
        at += w.shape[0]
    project((clusters,), weights, keys, values)
    columns = member[...].T
    lanes = lax.broadcasted_iota(jnp.int32, (TILE, clusters.shape[0]), 1)
    for t in range(count // TILE):
        here = pl.ds(t * TILE, TILE)
        q = own[here, :]
        one_hot = (columns[:, t : t + 1] == lanes).astype(BF16)
        own_cluster = dot(one_hot, clusters[...]).astype(BF16)
        base[here, :] = dot(q, weight(w_node, 0)) + dot(own_cluster, weight(w_node, 3))
        recv[here, :] = dot(q, w_in[:width, :])
        top[here, :], acc[here, :] = absorb(q, keys[...], values[...], None, None)


def edge_kernel(senders, own, xa, xb, ya, yb, za, zb, weights, recv, base, out, table, rows):
    count, _ = own.shape
    w_send = weight(weights, W_SEND)
    table[0:count, :] = dot(own[...], w_send)
    for at, axis, pair in ((0, "gx", (xa, xb)), (2, "gy", (ya, yb)), (4, "gz", (za, zb))):
        odd = lax.axis_index(axis) % 2
        low = pl.multiple_of(count + BND * (at + 1 - odd), BND)
        high = pl.multiple_of(count + BND * (at + odd), BND)
        table[pl.ds(low, BND), :] = dot(pair[0][:BND, :], w_send)
        table[pl.ds(high, BND), :] = dot(pair[1][:BND, :], w_send)
    w_sum = jnp.concatenate([weight(weights, W_MSG)] * 4, axis=0)

    def gather(g, _):
        for j in range(NODES_STEP):
            for d in range(4):
                index = senders[g * NODES_STEP * 4 + j * 4 + d]
                at = pl.multiple_of(g * NODES_STEP, NODES_STEP) + j
                rows[d, pl.ds(at, 1), :] = table[pl.ds(index, 1), :]
        return 0

    lax.fori_loop(0, count // NODES_STEP, gather, 0)
    hidden = jnp.concatenate([silu(rows[d] + recv[...]).astype(BF16) for d in range(4)], axis=1)
    agg = dot(hidden, w_sum).astype(BF16)
    out[...] = base[...] + dot(agg, weight(weights, W_AGG))


def middle_kernel(own, weights, top0, acc0, y0, y1, x0, x1, z0, z1, line_y, top_x, acc_x, top_z, acc_z, keys, values):
    count, width = own.shape
    n = x0.shape[0]
    project((y0.at[BND:, :], y1.at[BND:, :], x0, x1, z0, z1), weights, keys, values)

    for here in row_tiles(count, ROWS):
        q = own[here, :]
        t0, a0 = top0[here, :], acc0[here, :]
        _, a = absorb(q, keys[:, 0 : 3 * n], values[0 : 3 * n, :], t0, a0)
        line_y[here, :] = a[:, :width] / a[:, width:]
        top_x[here, :], acc_x[here, :] = absorb(q, keys[:, 3 * n : 6 * n], values[3 * n : 6 * n, :], t0, a0)
        top_z[here, :], acc_z[here, :] = absorb(q, keys[:, 6 * n : 9 * n], values[6 * n : 9 * n, :], t0, a0)


def final_kernel(
    own, weights, gain, base, line_y, top_x, acc_x, top_z, acc_z, x2, z2, out, keys, values, pooled
):
    count, width = own.shape
    n = x2.shape[0]
    project((x2, z2), weights, keys, values)
    for here in row_tiles(count, ROWS):
        q = own[here, :]
        _, ax = absorb(q, keys[:, 0:n], values[0:n, :], top_x[here, :], acc_x[here, :])
        _, az = absorb(q, keys[:, n : 2 * n], values[n : 2 * n, :], top_z[here, :], acc_z[here, :])
        pooled[here, :] = (
            line_y[here, :] + ax[:, :width] / ax[:, width:] + az[:, :width] / az[:, width:]
        )
    for here in row_tiles(count, 2 * ROWS):
        p = pooled[here, :]
        attended = (p * lax.rsqrt(jnp.mean(p * p, axis=1, keepdims=True) + 1e-06)).astype(BF16)
        preact = base[here, :] + dot(attended, weight(weights, W_ATT))
        update = dot(silu(preact).astype(BF16), weight(weights, W_OUT))
        centred = update - jnp.mean(update, axis=1, keepdims=True)
        variance = jnp.mean(centred * centred, axis=1, keepdims=True)
        normed = centred * lax.rsqrt(variance + 1e-05)
        out[here, :] = (own[here, :].astype(F32) + normed * gain[...]).astype(BF16)


def call(kernel, args, outs, scratch=(), scalars=(), local=True):
    space = pltpu.VMEM if local else jax.ShapeDtypeStruct
    many = isinstance(outs, list)
    return pl.pallas_call(
        kernel,
        out_shape=[space(*o) for o in outs] if many else space(*outs),
        in_specs=[SMEM] * len(scalars) + [VMEM] * len(args),
        out_specs=[VMEM] * len(outs) if many else VMEM,
        scratch_shapes=[pltpu.VMEM(*s) for s in scratch],
        compiler_params=pltpu.CompilerParams(vmem_limit_bytes=VMEM_BYTES),
    )(*scalars, *map(near, args))


def exchange(x, axis, partner):
    size = lax.axis_size(axis)
    return lax.ppermute(x, axis, [(i, partner(i) % size) for i in range(size)])


def other_side(i):
    return i + 1 if i % 2 else i - 1


def on_device(
    node_latents,
    cluster_latents,
    senders,
    membership,
    w_key,
    w_value,
    w_edge_in,
    w_edge_out,
    w_node_in,
    w_node_out,
    out_gain,
):
    count, width = node_latents.shape
    n = cluster_latents.shape[0]

    def stack(pieces):
        return call(stack_kernel, pieces, ((sum(p.shape[0] for p in pieces), width), BF16))

    z0 = exchange(cluster_latents, "gz", lambda i: i ^ 4)
    x0 = exchange(cluster_latents, "gx", lambda i: i ^ 2)
    own, clusters, border, both, member, gain = pl.pallas_call(
        load_kernel,
        out_shape=[
            pltpu.VMEM((count, width), BF16),
            pltpu.VMEM((n, width), BF16),
            pltpu.VMEM((BND, width), BF16),
            pltpu.VMEM((BND + n, width), BF16),
            pltpu.VMEM((count // TILE, TILE), jnp.int32),
            pltpu.VMEM((1, width), F32),
        ],
        in_specs=[pl.BlockSpec(memory_space=pltpu.HBM)] * 4,
        out_specs=[VMEM] * 6,
        scratch_shapes=[pltpu.SemaphoreType.DMA((7,))],
        compiler_params=pltpu.CompilerParams(vmem_limit_bytes=VMEM_BYTES),
        name="load",
    )(
        *(
            pltpu.with_memory_space_constraint(x, pltpu.HBM)
            for x in (
                node_latents,
                cluster_latents,
                membership.reshape(count // TILE, TILE),
                out_gain.reshape(1, width),
            )
        )
    )
    y0 = exchange(both, "gy", lambda i: i ^ 1)
    za = exchange(border, "gz", lambda i: i ^ 1)
    xa = exchange(border, "gx", lambda i: i ^ 1)
    zb = exchange(border, "gz", other_side)
    xb = exchange(border, "gx", other_side)

    weights, recv, base, top, acc = call(
        prep_kernel,
        (
            own,
            clusters,
            member,
            w_key,
            w_value,
            w_edge_in,
            w_edge_out,
            w_node_in,
            w_node_out,
        ),
        [
            ((10 * width, width), BF16),
            ((count, width), F32),
            ((count, width), F32),
            ((count, width), F32),
            ((count, 2 * width), F32),
        ],
        [((width, n), BF16), ((n, 2 * width), BF16)],
    )

    x1 = exchange(stack((clusters, x0)), "gx", lambda i: i ^ 4)
    y1 = exchange(
        call(stack_after_border_kernel, (border, clusters, y0), ((BND + 2 * n, width), BF16)),
        "gy",
        lambda i: i ^ 3,
    )
    z1 = exchange(stack((clusters, z0)), "gz", lambda i: i ^ 2)
    z2 = exchange(stack((clusters, z0, z1)), "gz", lambda i: i ^ 1)
    x2 = exchange(stack((clusters, x0, x1)), "gx", lambda i: i ^ 1)

    base = call(
        edge_kernel,
        (own, xa, xb, y0, y1, za, zb, weights, recv, base),
        ((count, width), F32),
        [((count + 6 * BND, width), F32), ((4, count, width), F32)],
        (senders.reshape(-1),),
    )
    line_y, top_x, acc_x, top_z, acc_z = call(
        middle_kernel,
        (own, weights, top, acc, y0, y1, x0, x1, z0, z1),
        [((count, width), F32)] + [((count, width), F32), ((count, 2 * width), F32)] * 2,
        [((width, 9 * n), BF16), ((9 * n, 2 * width), BF16)],
    )
    return call(
        final_kernel,
        (own, weights, gain, base, line_y, top_x, acc_x, top_z, acc_z, x2, z2),
        ((count, width), BF16),
        [((width, 8 * n), BF16), ((8 * n, 2 * width), BF16), ((count, width), F32)],
        local=False,
    )


def solution(mesh):
    split = P(("gx", "gy", "gz"), None)
    in_specs = (split, split, split, P(("gx", "gy", "gz"))) + (P(),) * 7

    return jax.shard_map(on_device, mesh=mesh, in_specs=in_specs, out_specs=split, check_vma=False)
```

```python
import math

import jax
import jax.numpy as jnp
from jax import lax
from jax.experimental import pallas as pl
from jax.experimental.pallas import tpu as pltpu
from jax.sharding import PartitionSpec as P


BND = 512
F32 = jnp.float32
BF16 = jnp.bfloat16
TILE = 128
ROWS = 256
VMEM_BYTES = 20 * 2**20

VMEM = pl.BlockSpec(memory_space=pltpu.VMEM)
SMEM = pl.BlockSpec(memory_space=pltpu.SMEM)

W_KEY, W_VALUE, _, W_SEND, W_MSG, _, W_AGG, W_ATT, _, W_OUT = range(10)


def near(x):
    return pltpu.with_memory_space_constraint(x, pltpu.VMEM)


def dot(a, b):
    return jnp.dot(a, b, preferred_element_type=F32)


def silu(x):
    return x * 0.5 * (1.0 + jnp.tanh(x * 0.5))


def weight(stacked, which):
    width = stacked.shape[1]
    return stacked[which * width : (which + 1) * width, :]


def scale_of(width):
    return math.log2(math.e) / math.sqrt(width)


def row_tiles(count, rows):
    return [pl.ds(at, rows) for at in range(0, count, rows)]


def project(pieces, weights, keys, values):
    width = weights.shape[1]
    at = 0
    for piece in pieces:
        n = piece.shape[0]
        keys[:, at : at + n] = dot(piece[...], weight(weights, W_KEY)).astype(BF16).T
        values[at : at + n, 0:width] = dot(piece[...], weight(weights, W_VALUE)).astype(BF16)
        values[at : at + n, width : 2 * width] = jnp.ones((n, width), BF16)
        at += n


def wide(x, copies):
    return jnp.concatenate([x] * copies, axis=1)


def absorb(q, keys, values, top, acc):
    width = q.shape[1]
    scale = scale_of(width)
    scores = dot(q, keys)
    highest = jnp.broadcast_to(jnp.max(scores, axis=1, keepdims=True), (q.shape[0], width))
    newest = highest if top is None else jnp.maximum(top, highest)
    weights = jnp.exp2((scores - wide(newest, scores.shape[1] // width)) * scale).astype(BF16)
    part = dot(weights, values)
    if top is not None:
        part = acc * wide(jnp.exp2((top - newest) * scale), 2) + part
    return newest, part


def load_kernel(
    own_far, clusters_far, member_far, gain_far, own, clusters, border, both, member, gain, done
):
    head = own_far.at[:BND, :]
    copies = [
        pltpu.make_async_copy(source, target, done.at[at])
        for at, (source, target) in enumerate(
            (
                (head, both.at[:BND, :]),
                (clusters_far, both.at[BND:, :]),
                (head, border),
                (clusters_far, clusters),
                (member_far, member),
                (gain_far, gain),
                (own_far, own),
            )
        )
    ]
    for copy in copies:
        copy.start()
    for copy in copies:
        copy.wait()


def stack_kernel(*refs):
    *pieces, out = refs
    at = 0
    for piece in pieces:
        out[at : at + piece.shape[0], :] = piece[...]
        at += piece.shape[0]


def stack_after_border_kernel(border, clusters, came, out):
    n = clusters.shape[0]
    out[:BND, :] = border[...]
    out[BND : BND + n, :] = clusters[...]
    out[BND + n :, :] = came[BND:, :]


def prep_kernel(
    own, clusters, member, w_key, w_value, w_in, w_msg, w_node, w_out,
    weights, recv, base, top, acc, keys, values,
):
    count, width = own.shape
    at = 0
    for w in (w_key, w_value, w_in, w_msg, w_node, w_out):
        weights[at : at + w.shape[0], :] = w[...]
        at += w.shape[0]
    project((clusters,), weights, keys, values)
    columns = member[...].T
    lanes = lax.broadcasted_iota(jnp.int32, (TILE, clusters.shape[0]), 1)
    for t in range(count // TILE):
        here = pl.ds(t * TILE, TILE)
        q = own[here, :]
        one_hot = (columns[:, t : t + 1] == lanes).astype(BF16)
        own_cluster = dot(one_hot, clusters[...]).astype(BF16)
        base[here, :] = dot(q, weight(w_node, 0)) + dot(own_cluster, weight(w_node, 3))
        recv[here, :] = dot(q, w_in[:width, :])
        top[here, :], acc[here, :] = absorb(q, keys[...], values[...], None, None)


def work_kernel(
    senders, own, xa, xb, za, zb, weights, recv, base, top0, acc0, y0, y1, x0, x1, z0, z1,
    node_part, line_y, top_x, acc_x, top_z, acc_z, table, rows, keys, values,
):
    count, width = own.shape
    n = x0.shape[0]
    w_send = weight(weights, W_SEND)
    table[0:count, :] = dot(own[...], w_send)
    for at, axis, pair in ((0, "gx", (xa, xb)), (2, "gy", (y0, y1)), (4, "gz", (za, zb))):
        odd = lax.axis_index(axis) % 2
        low = pl.multiple_of(count + BND * (at + 1 - odd), BND)
        high = pl.multiple_of(count + BND * (at + odd), BND)
        table[pl.ds(low, BND), :] = dot(pair[0][:BND, :], w_send)
        table[pl.ds(high, BND), :] = dot(pair[1][:BND, :], w_send)
    w_sum = jnp.concatenate([weight(weights, W_MSG)] * 4, axis=0)
    project((y0.at[BND:, :], y1.at[BND:, :], x0, x1, z0, z1), weights, keys, values)

    def gather(first, nodes):
        for node in range(first, first + nodes):
            for d in range(4):
                rows[d, node : node + 1, :] = table[pl.ds(senders[4 * node + d], 1), :]

    def line(here, at):
        return absorb(
            own[here, :], keys[:, at : at + 3 * n], values[at : at + 3 * n, :], top0[here, :], acc0[here, :]
        )

    for here in row_tiles(count, ROWS):
        gather(here.start, ROWS // 2)
        _, a = line(here, 0)
        line_y[here, :] = a[:, :width] / a[:, width:]
        gather(here.start + ROWS // 2, ROWS // 2)
        top_x[here, :], acc_x[here, :] = line(here, 3 * n)
        top_z[here, :], acc_z[here, :] = line(here, 6 * n)
        hidden = jnp.concatenate(
            [silu(rows[d, here, :] + recv[here, :]).astype(BF16) for d in range(4)], axis=1
        )
        agg = dot(hidden, w_sum).astype(BF16)
        node_part[here, :] = base[here, :] + dot(agg, weight(weights, W_AGG))


def final_kernel(
    own, weights, gain, base, line_y, top_x, acc_x, top_z, acc_z, x2, z2, out, keys, values, pooled
):
    count, width = own.shape
    n = x2.shape[0]
    project((x2, z2), weights, keys, values)
    for here in row_tiles(count, ROWS):
        q = own[here, :]
        _, ax = absorb(q, keys[:, 0:n], values[0:n, :], top_x[here, :], acc_x[here, :])
        _, az = absorb(q, keys[:, n : 2 * n], values[n : 2 * n, :], top_z[here, :], acc_z[here, :])
        pooled[here, :] = (
            line_y[here, :] + ax[:, :width] / ax[:, width:] + az[:, :width] / az[:, width:]
        )
    for here in row_tiles(count, 2 * ROWS):
        p = pooled[here, :]
        attended = (p * lax.rsqrt(jnp.mean(p * p, axis=1, keepdims=True) + 1e-06)).astype(BF16)
        preact = base[here, :] + dot(attended, weight(weights, W_ATT))
        update = dot(silu(preact).astype(BF16), weight(weights, W_OUT))
        centred = update - jnp.mean(update, axis=1, keepdims=True)
        variance = jnp.mean(centred * centred, axis=1, keepdims=True)
        normed = centred * lax.rsqrt(variance + 1e-05)
        out[here, :] = (own[here, :].astype(F32) + normed * gain[...]).astype(BF16)


def call(kernel, args, outs, scratch=(), scalars=(), local=True):
    space = pltpu.VMEM if local else jax.ShapeDtypeStruct
    many = isinstance(outs, list)
    return pl.pallas_call(
        kernel,
        out_shape=[space(*o) for o in outs] if many else space(*outs),
        in_specs=[SMEM] * len(scalars) + [VMEM] * len(args),
        out_specs=[VMEM] * len(outs) if many else VMEM,
        scratch_shapes=[pltpu.VMEM(*s) for s in scratch],
        compiler_params=pltpu.CompilerParams(vmem_limit_bytes=VMEM_BYTES),
    )(*scalars, *map(near, args))


def exchange(x, axis, partner):
    size = lax.axis_size(axis)
    return lax.ppermute(x, axis, [(i, partner(i) % size) for i in range(size)])


def other_side(i):
    return i + 1 if i % 2 else i - 1


def on_device(
    node_latents,
    cluster_latents,
    senders,
    membership,
    w_key,
    w_value,
    w_edge_in,
    w_edge_out,
    w_node_in,
    w_node_out,
    out_gain,
):
    count, width = node_latents.shape
    n = cluster_latents.shape[0]

    def stack(pieces):
        return call(stack_kernel, pieces, ((sum(p.shape[0] for p in pieces), width), BF16))

    z0 = exchange(cluster_latents, "gz", lambda i: i ^ 4)
    x0 = exchange(cluster_latents, "gx", lambda i: i ^ 2)
    own, clusters, border, both, member, gain = pl.pallas_call(
        load_kernel,
        out_shape=[
            pltpu.VMEM((count, width), BF16),
            pltpu.VMEM((n, width), BF16),
            pltpu.VMEM((BND, width), BF16),
            pltpu.VMEM((BND + n, width), BF16),
            pltpu.VMEM((count // TILE, TILE), jnp.int32),
            pltpu.VMEM((1, width), F32),
        ],
        in_specs=[pl.BlockSpec(memory_space=pltpu.HBM)] * 4,
        out_specs=[VMEM] * 6,
        scratch_shapes=[pltpu.SemaphoreType.DMA((7,))],
        compiler_params=pltpu.CompilerParams(vmem_limit_bytes=VMEM_BYTES),
        name="load",
    )(
        *(
            pltpu.with_memory_space_constraint(x, pltpu.HBM)
            for x in (
                node_latents,
                cluster_latents,
                membership.reshape(count // TILE, TILE),
                out_gain.reshape(1, width),
            )
        )
    )
    y0 = exchange(both, "gy", lambda i: i ^ 1)
    za = exchange(border, "gz", lambda i: i ^ 1)
    xa = exchange(border, "gx", lambda i: i ^ 1)
    zb = exchange(border, "gz", other_side)
    xb = exchange(border, "gx", other_side)

    weights, recv, base, top, acc = call(
        prep_kernel,
        (
            own,
            clusters,
            member,
            w_key,
            w_value,
            w_edge_in,
            w_edge_out,
            w_node_in,
            w_node_out,
        ),
        [
            ((10 * width, width), BF16),
            ((count, width), F32),
            ((count, width), F32),
            ((count, width), F32),
            ((count, 2 * width), F32),
        ],
        [((width, n), BF16), ((n, 2 * width), BF16)],
    )

    x1 = exchange(stack((clusters, x0)), "gx", lambda i: i ^ 4)
    y1 = exchange(
        call(stack_after_border_kernel, (border, clusters, y0), ((BND + 2 * n, width), BF16)),
        "gy",
        lambda i: i ^ 3,
    )
    z1 = exchange(stack((clusters, z0)), "gz", lambda i: i ^ 2)
    z2 = exchange(stack((clusters, z0, z1)), "gz", lambda i: i ^ 1)
    x2 = exchange(stack((clusters, x0, x1)), "gx", lambda i: i ^ 1)

    base, line_y, top_x, acc_x, top_z, acc_z = call(
        work_kernel,
        (own, xa, xb, za, zb, weights, recv, base, top, acc, y0, y1, x0, x1, z0, z1),
        [((count, width), F32)] * 2 + [((count, width), F32), ((count, 2 * width), F32)] * 2,
        [
            ((count + 6 * BND, width), F32),
            ((4, count, width), F32),
            ((width, 9 * n), BF16),
            ((9 * n, 2 * width), BF16),
        ],
        (senders.reshape(-1),),
    )
    return call(
        final_kernel,
        (own, weights, gain, base, line_y, top_x, acc_x, top_z, acc_z, x2, z2),
        ((count, width), BF16),
        [((width, 8 * n), BF16), ((8 * n, 2 * width), BF16), ((count, width), F32)],
        local=False,
    )


def solution(mesh):
    split = P(("gx", "gy", "gz"), None)
    in_specs = (split, split, split, P(("gx", "gy", "gz"))) + (P(),) * 7

    return jax.shard_map(on_device, mesh=mesh, in_specs=in_specs, out_specs=split, check_vma=False)
```

```python
import math

import jax
import jax.numpy as jnp
from jax import lax
from jax.experimental import pallas as pl
from jax.experimental.pallas import tpu as pltpu
from jax.sharding import PartitionSpec as P


BND = 512
F32 = jnp.float32
BF16 = jnp.bfloat16
TILE = 128
ROWS = 256
VMEM_BYTES = 20 * 2**20

VMEM = pl.BlockSpec(memory_space=pltpu.VMEM)
SMEM = pl.BlockSpec(memory_space=pltpu.SMEM)

W_KEY, W_VALUE, _, W_SEND, W_MSG, _, W_AGG, W_ATT, _, W_OUT = range(10)


def near(x):
    return pltpu.with_memory_space_constraint(x, pltpu.VMEM)


def dot(a, b):
    return jnp.dot(a, b, preferred_element_type=F32)


def silu(x):
    return x * 0.5 * (1.0 + jnp.tanh(x * 0.5))


def weight(stacked, which):
    width = stacked.shape[1]
    return stacked[which * width : (which + 1) * width, :]


def scale_of(width):
    return math.log2(math.e) / math.sqrt(width)


def row_tiles(count, rows):
    return [pl.ds(at, rows) for at in range(0, count, rows)]


def project(pieces, weights, keys, values):
    width = weights.shape[1]
    at = 0
    for piece in pieces:
        n = piece.shape[0]
        keys[:, at : at + n] = dot(piece[...], weight(weights, W_KEY)).astype(BF16).T
        values[at : at + n, 0:width] = dot(piece[...], weight(weights, W_VALUE)).astype(BF16)
        values[at : at + n, width : 2 * width] = jnp.ones((n, width), BF16)
        at += n


def wide(x, copies):
    return jnp.concatenate([x] * copies, axis=1)


def absorb(q, keys, values, top, acc):
    width = q.shape[1]
    scale = scale_of(width)
    scores = dot(q, keys)
    highest = jnp.broadcast_to(jnp.max(scores, axis=1, keepdims=True), (q.shape[0], width))
    newest = highest if top is None else jnp.maximum(top, highest)
    weights = jnp.exp2((scores - wide(newest, scores.shape[1] // width)) * scale).astype(BF16)
    part = dot(weights, values)
    if top is not None:
        part = acc * wide(jnp.exp2((top - newest) * scale), 2) + part
    return newest, part


def load_kernel(
    own_far, clusters_far, member_far, gain_far, own, clusters, border, both, member, gain, done
):
    head = own_far.at[:BND, :]
    copies = [
        pltpu.make_async_copy(source, target, done.at[at])
        for at, (source, target) in enumerate(
            (
                (head, both.at[:BND, :]),
                (clusters_far, both.at[BND:, :]),
                (head, border),
                (clusters_far, clusters),
                (member_far, member),
                (gain_far, gain),
                (own_far, own),
            )
        )
    ]
    for copy in copies:
        copy.start()
    for copy in copies:
        copy.wait()


def stack_kernel(*refs):
    *pieces, out = refs
    at = 0
    for piece in pieces:
        out[at : at + piece.shape[0], :] = piece[...]
        at += piece.shape[0]


def stack_after_border_kernel(border, clusters, came, out):
    n = clusters.shape[0]
    out[:BND, :] = border[...]
    out[BND : BND + n, :] = clusters[...]
    out[BND + n :, :] = came[BND:, :]


def prep_kernel(
    own, clusters, member, w_key, w_value, w_in, w_msg, w_node, w_out,
    weights, recv, base, top, acc, keys, values,
):
    count, width = own.shape
    at = 0
    for w in (w_key, w_value, w_in, w_msg, w_node, w_out):
        weights[at : at + w.shape[0], :] = w[...]
        at += w.shape[0]
    project((clusters,), weights, keys, values)
    columns = member[...].T
    lanes = lax.broadcasted_iota(jnp.int32, (TILE, clusters.shape[0]), 1)
    for t in range(count // TILE):
        here = pl.ds(t * TILE, TILE)
        q = own[here, :]
        one_hot = (columns[:, t : t + 1] == lanes).astype(BF16)
        own_cluster = dot(one_hot, clusters[...]).astype(BF16)
        base[here, :] = dot(q, weight(w_node, 0)) + dot(own_cluster, weight(w_node, 3))
        recv[here, :] = dot(q, w_in[:width, :])
        top[here, :], acc[here, :] = absorb(q, keys[...], values[...], None, None)


def line_y_kernel(own, weights, top0, acc0, y0, y1, line_y, keys, values):
    count, width = own.shape
    project((y0.at[BND:, :], y1.at[BND:, :]), weights, keys, values)
    for here in row_tiles(count, ROWS):
        _, a = absorb(own[here, :], keys[...], values[...], top0[here, :], acc0[here, :])
        line_y[here, :] = a[:, :width] / a[:, width:]


def work_kernel(
    senders, own, xa, xb, za, zb, weights, recv, base, top0, acc0, y0, y1, x0, x1, z0, z1,
    node_part, top_x, acc_x, top_z, acc_z, table, rows, keys, values,
):
    count, _ = own.shape
    n = x0.shape[0]
    w_send = weight(weights, W_SEND)
    table[0:count, :] = dot(own[...], w_send)
    for at, axis, pair in ((0, "gx", (xa, xb)), (2, "gy", (y0, y1)), (4, "gz", (za, zb))):
        odd = lax.axis_index(axis) % 2
        low = pl.multiple_of(count + BND * (at + 1 - odd), BND)
        high = pl.multiple_of(count + BND * (at + odd), BND)
        table[pl.ds(low, BND), :] = dot(pair[0][:BND, :], w_send)
        table[pl.ds(high, BND), :] = dot(pair[1][:BND, :], w_send)
    w_sum = jnp.concatenate([weight(weights, W_MSG)] * 4, axis=0)
    project((x0, x1, z0, z1), weights, keys, values)

    def gather(first, nodes):
        for node in range(first, first + nodes):
            for d in range(4):
                rows[d, node : node + 1, :] = table[pl.ds(senders[4 * node + d], 1), :]

    def line(here, at):
        return absorb(
            own[here, :], keys[:, at : at + 3 * n], values[at : at + 3 * n, :], top0[here, :], acc0[here, :]
        )

    for here in row_tiles(count, ROWS):
        gather(here.start, ROWS // 2)
        top_x[here, :], acc_x[here, :] = line(here, 0)
        gather(here.start + ROWS // 2, ROWS // 2)
        top_z[here, :], acc_z[here, :] = line(here, 3 * n)
        hidden = jnp.concatenate(
            [silu(rows[d, here, :] + recv[here, :]).astype(BF16) for d in range(4)], axis=1
        )
        agg = dot(hidden, w_sum).astype(BF16)
        node_part[here, :] = base[here, :] + dot(agg, weight(weights, W_AGG))


def final_kernel(
    own, weights, gain, base, line_y, top_x, acc_x, top_z, acc_z, x2, z2, out, keys, values, pooled
):
    count, width = own.shape
    n = x2.shape[0]
    project((x2, z2), weights, keys, values)
    for here in row_tiles(count, ROWS):
        q = own[here, :]
        _, ax = absorb(q, keys[:, 0:n], values[0:n, :], top_x[here, :], acc_x[here, :])
        _, az = absorb(q, keys[:, n : 2 * n], values[n : 2 * n, :], top_z[here, :], acc_z[here, :])
        pooled[here, :] = (
            line_y[here, :] + ax[:, :width] / ax[:, width:] + az[:, :width] / az[:, width:]
        )
    for here in row_tiles(count, 2 * ROWS):
        p = pooled[here, :]
        attended = (p * lax.rsqrt(jnp.mean(p * p, axis=1, keepdims=True) + 1e-06)).astype(BF16)
        preact = base[here, :] + dot(attended, weight(weights, W_ATT))
        update = dot(silu(preact).astype(BF16), weight(weights, W_OUT))
        centred = update - jnp.mean(update, axis=1, keepdims=True)
        variance = jnp.mean(centred * centred, axis=1, keepdims=True)
        normed = centred * lax.rsqrt(variance + 1e-05)
        out[here, :] = (own[here, :].astype(F32) + normed * gain[...]).astype(BF16)


def call(kernel, args, outs, scratch=(), scalars=(), local=True):
    space = pltpu.VMEM if local else jax.ShapeDtypeStruct
    many = isinstance(outs, list)
    return pl.pallas_call(
        kernel,
        out_shape=[space(*o) for o in outs] if many else space(*outs),
        in_specs=[SMEM] * len(scalars) + [VMEM] * len(args),
        out_specs=[VMEM] * len(outs) if many else VMEM,
        scratch_shapes=[pltpu.VMEM(*s) for s in scratch],
        compiler_params=pltpu.CompilerParams(vmem_limit_bytes=VMEM_BYTES),
    )(*scalars, *map(near, args))


def exchange(x, axis, partner):
    size = lax.axis_size(axis)
    return lax.ppermute(x, axis, [(i, partner(i) % size) for i in range(size)])


def other_side(i):
    return i + 1 if i % 2 else i - 1


def on_device(
    node_latents,
    cluster_latents,
    senders,
    membership,
    w_key,
    w_value,
    w_edge_in,
    w_edge_out,
    w_node_in,
    w_node_out,
    out_gain,
):
    count, width = node_latents.shape
    n = cluster_latents.shape[0]

    def stack(pieces):
        return call(stack_kernel, pieces, ((sum(p.shape[0] for p in pieces), width), BF16))

    z0 = exchange(cluster_latents, "gz", lambda i: i ^ 4)
    x0 = exchange(cluster_latents, "gx", lambda i: i ^ 4)
    own, clusters, border, both, member, gain = pl.pallas_call(
        load_kernel,
        out_shape=[
            pltpu.VMEM((count, width), BF16),
            pltpu.VMEM((n, width), BF16),
            pltpu.VMEM((BND, width), BF16),
            pltpu.VMEM((BND + n, width), BF16),
            pltpu.VMEM((count // TILE, TILE), jnp.int32),
            pltpu.VMEM((1, width), F32),
        ],
        in_specs=[pl.BlockSpec(memory_space=pltpu.HBM)] * 4,
        out_specs=[VMEM] * 6,
        scratch_shapes=[pltpu.SemaphoreType.DMA((7,))],
        compiler_params=pltpu.CompilerParams(vmem_limit_bytes=VMEM_BYTES),
        name="load",
    )(
        *(
            pltpu.with_memory_space_constraint(x, pltpu.HBM)
            for x in (
                node_latents,
                cluster_latents,
                membership.reshape(count // TILE, TILE),
                out_gain.reshape(1, width),
            )
        )
    )
    y0 = exchange(both, "gy", lambda i: i ^ 1)
    za = exchange(border, "gz", lambda i: i ^ 1)
    xa = exchange(border, "gx", lambda i: i ^ 1)
    zb = exchange(border, "gz", other_side)
    xb = exchange(border, "gx", other_side)

    weights, recv, base, top, acc = call(
        prep_kernel,
        (
            own,
            clusters,
            member,
            w_key,
            w_value,
            w_edge_in,
            w_edge_out,
            w_node_in,
            w_node_out,
        ),
        [
            ((10 * width, width), BF16),
            ((count, width), F32),
            ((count, width), F32),
            ((count, width), F32),
            ((count, 2 * width), F32),
        ],
        [((width, n), BF16), ((n, 2 * width), BF16)],
    )

    x1 = exchange(stack((clusters, x0)), "gx", lambda i: i ^ 2)
    y1 = exchange(
        call(stack_after_border_kernel, (border, clusters, y0), ((BND + 2 * n, width), BF16)),
        "gy",
        lambda i: i ^ 3,
    )
    z1 = exchange(stack((clusters, z0)), "gz", lambda i: i ^ 2)
    z2 = exchange(stack((clusters, z0, z1)), "gz", lambda i: i ^ 1)
    x2 = exchange(stack((clusters, x0, x1)), "gx", lambda i: i ^ 1)

    line_y = call(
        line_y_kernel,
        (own, weights, top, acc, y0, y1),
        ((count, width), F32),
        [((width, 3 * n), BF16), ((3 * n, 2 * width), BF16)],
    )
    base, top_x, acc_x, top_z, acc_z = call(
        work_kernel,
        (own, xa, xb, za, zb, weights, recv, base, top, acc, y0, y1, x0, x1, z0, z1),
        [((count, width), F32)] + [((count, width), F32), ((count, 2 * width), F32)] * 2,
        [
            ((count + 6 * BND, width), F32),
            ((4, count, width), F32),
            ((width, 6 * n), BF16),
            ((6 * n, 2 * width), BF16),
        ],
        (senders.reshape(-1),),
    )
    return call(
        final_kernel,
        (own, weights, gain, base, line_y, top_x, acc_x, top_z, acc_z, x2, z2),
        ((count, width), BF16),
        [((width, 8 * n), BF16), ((8 * n, 2 * width), BF16), ((count, width), F32)],
        local=False,
    )


def solution(mesh):
    split = P(("gx", "gy", "gz"), None)
    in_specs = (split, split, split, P(("gx", "gy", "gz"))) + (P(),) * 7

    return jax.shard_map(on_device, mesh=mesh, in_specs=in_specs, out_specs=split, check_vma=False)
```
